32 devices in a mesh: dp: 1 (over z), ep: 32 (over y, x, core).
Axes of the slice: x: 4, y: 4, z: 1, core: 2. Of those that a mesh axis runs over, the one named last changes fastest.
The devices are a block of a 4x4x8 slice.
Arguments:
- tokens: bfloat16 [16384, 2048], P(('dp', 'ep'))
- route_idx: int32 [16384, 6], P(('dp', 'ep'))
- gate_vals: float32 [16384, 6], P(('dp', 'ep'))
- w_gate: bfloat16 [64, 2048, 1408], P('ep')
- w_up: bfloat16 [64, 2048, 1408], P('ep')
- w_down: bfloat16 [64, 1408, 2048], P('ep')
Outputs:
- output: bfloat16 [16384, 2048], P(('dp', 'ep'))
All inputs are finite; a program needn't handle non-finite values.
Results may differ from the reference program's by a relative error of at most 0.00786291.
Values are sent between devices in bfloat16 or wider.
A program may use at most 768 MiB of HBM per device.

```python
import functools
import jax
import jax.numpy as jnp
from jax import lax

TOKENS_DEV = 512
GROUP_SIZE = 32
D_MODEL = 2048
D_FF = 1408
EXPERTS = 64
TOP_K = 6
CAPACITY = 256
TOKENS = TOKENS_DEV * GROUP_SIZE


def device_routing(expert_order, hot_counts, dev_key):
    key_jitter, key_perm, key_tokens = jax.random.split(dev_key, 3)
    cold_n = EXPERTS - TOP_K
    half_n = cold_n // 2
    rest_slots = TOKENS_DEV * TOP_K - jnp.sum(hot_counts)
    base_count = rest_slots // cold_n
    extra_count = rest_slots - base_count * cold_n
    cold_counts = base_count + (jnp.arange(cold_n) < extra_count).astype(jnp.int32)
    jitter_up = jax.random.randint(key_jitter, (half_n,), 0, (base_count - 1) // 2 + 1)
    jitter = jnp.stack([jitter_up, -jitter_up], axis=1).reshape(-1)
    jitter = jnp.pad(jitter, (0, cold_n - 2 * half_n))
    cold_counts = cold_counts + jax.random.permutation(key_perm, jitter)
    all_counts = jnp.concatenate([hot_counts, cold_counts])
    run_ends = jnp.cumsum(all_counts)
    rank_ids = jnp.searchsorted(run_ends, jnp.arange(TOKENS_DEV * TOP_K), side="right")
    flat_ids = expert_order[rank_ids]
    slot_grid = flat_ids.reshape(TOP_K, TOKENS_DEV).T
    return jax.random.permutation(key_tokens, slot_grid, axis=0)


def draw_routing(route_key):
    key_order, key_hot, key_pick, key_dev = jax.random.split(route_key, 4)
    expert_order = jax.random.permutation(key_order, EXPERTS)
    hot_counts = CAPACITY - jax.random.randint(key_hot, (GROUP_SIZE, TOP_K), 0, CAPACITY // 4 + 1)
    full_dev = jax.random.randint(key_pick, (), 0, GROUP_SIZE)
    at_full = (jnp.arange(GROUP_SIZE)[:, None] == full_dev) & (jnp.arange(TOP_K)[None, :] == 0)
    hot_counts = jnp.where(at_full, CAPACITY, hot_counts)
    dev_keys = jax.random.split(key_dev, GROUP_SIZE)
    per_device = jax.vmap(functools.partial(device_routing, expert_order))(hot_counts, dev_keys)
    return per_device.reshape(TOKENS, TOP_K).astype(jnp.int32)


def draw_weight(weight_key, fan_in, fan_out):
    expert_keys = jax.random.split(weight_key, EXPERTS)
    return lax.map(lambda one_key: (jax.random.normal(one_key, (fan_in, fan_out), jnp.float32) * fan_in ** -0.5).astype(jnp.bfloat16), expert_keys)


def setup_inputs(seed: int = 0, part: int = 0) -> dict:
    root_key = jax.random.key(seed)
    part_key = jax.random.fold_in(root_key, part)
    key_tok, key_route, key_gate = jax.random.split(part_key, 3)
    key_wg, key_wu, key_wd = jax.random.split(jax.random.key(seed + 1), 3)
    tokens = jax.random.normal(key_tok, (TOKENS, D_MODEL), jnp.float32).astype(jnp.bfloat16)
    route_idx = draw_routing(key_route)
    gate_vals = jax.random.uniform(key_gate, (TOKENS, TOP_K), jnp.float32, 0.5, 1.5) * TOP_K ** -0.5
    return {"tokens": tokens, "route_idx": route_idx, "gate_vals": gate_vals, "w_gate": draw_weight(key_wg, D_MODEL, D_FF), "w_up": draw_weight(key_wu, D_MODEL, D_FF), "w_down": draw_weight(key_wd, D_FF, D_MODEL)}


def reference(tokens, route_idx, gate_vals, w_gate, w_up, w_down):
    row_cap = GROUP_SIZE * CAPACITY
    targets = jnp.arange(row_cap) + 1

    def expert_step(y_acc, expert_args):
        expert_id, wg_one, wu_one, wd_one = expert_args
        hit_mask = route_idx == expert_id
        member = jnp.sum(hit_mask, axis=1, dtype=jnp.int32)
        row_weight = jnp.sum(jnp.where(hit_mask, gate_vals, 0.0), axis=1)
        row_ids = jnp.searchsorted(jnp.cumsum(member), targets, side="left")
        picked = jnp.take(tokens, row_ids, axis=0, mode="fill", fill_value=0)
        pre_gate = jnp.dot(picked, wg_one, preferred_element_type=jnp.float32)
        pre_up = jnp.dot(picked, wu_one, preferred_element_type=jnp.float32)
        hidden = (jax.nn.silu(pre_gate) * pre_up).astype(jnp.bfloat16)
        expert_out = jnp.dot(hidden, wd_one, preferred_element_type=jnp.float32).astype(jnp.bfloat16)
        row_gate = jnp.take(row_weight, row_ids, mode="fill", fill_value=0.0)
        y_acc = y_acc.at[row_ids].add(row_gate[:, None] * expert_out.astype(jnp.float32), mode="drop")
        return y_acc, None

    y_init = jnp.zeros((TOKENS, D_MODEL), jnp.float32)
    y_sum, unused = lax.scan(expert_step, y_init, (jnp.arange(EXPERTS), w_gate, w_up, w_down))
    return y_sum.astype(jnp.bfloat16)
```

```python
import functools

import jax
import jax.numpy as jnp
from jax import lax
from jax.experimental import pallas as pl
from jax.experimental.pallas import tpu as pltpu
from jax.sharding import PartitionSpec as P

CHUNKS = 4
GROUP = 512
TILE = 256
SMALL = 64


def expert_kernel(counts, x_ref, pos_ref, gate_ref, wg_ref, wu_ref, wd_ref, out_ref):
    step = pl.program_id(0)
    local_n = wg_ref.shape[0]
    out_ref[...] = jnp.zeros_like(out_ref)

    def run_tile(expert, first, rows):
        ranks = pos_ref[0, expert : expert + 1, :] - first
        row_id = lax.broadcasted_iota(jnp.int32, (rows, ranks.shape[1]), 0)
        pick = jnp.where(row_id == ranks, 1.0, 0.0).astype(jnp.bfloat16)
        picked = jnp.dot(pick, x_ref[...], preferred_element_type=jnp.float32).astype(jnp.bfloat16)
        pre_gate = jnp.dot(picked, wg_ref[expert], preferred_element_type=jnp.float32)
        pre_up = jnp.dot(picked, wu_ref[expert], preferred_element_type=jnp.float32)
        hidden = (jax.nn.silu(pre_gate) * pre_up).astype(jnp.bfloat16)
        rows_out = jnp.dot(hidden, wd_ref[expert], preferred_element_type=jnp.float32).astype(jnp.bfloat16)
        placed = lax.dot_general(pick, rows_out, (((0,), (0,)), ((), ())), preferred_element_type=jnp.float32)
        out_ref[...] += gate_ref[:, expert : expert + 1] * placed

    for expert in range(local_n):
        count = counts[step, expert]

        @pl.when((count > 0) & (count <= SMALL))
        def _():
            run_tile(expert, 0, SMALL)

        @pl.when(count > SMALL)
        def _():
            def body(tile, carry):
                run_tile(expert, tile * TILE, TILE)
                return carry

            lax.fori_loop(0, (count + TILE - 1) // TILE, body, 0)


def run_experts(x_rows, ranks, gates, counts, wg_loc, wu_loc, wd_loc):
    n_rows, d_model = x_rows.shape
    local_n, _, d_ff = wg_loc.shape
    groups = n_rows // GROUP
    whole = functools.partial(pl.BlockSpec, pipeline_mode=pl.Buffered(1))
    return pl.pallas_call(
        expert_kernel,
        out_shape=jax.ShapeDtypeStruct((n_rows, d_model), jnp.float32),
        grid_spec=pltpu.PrefetchScalarGridSpec(
            num_scalar_prefetch=1,
            grid=(groups,),
            in_specs=[
                pl.BlockSpec((GROUP, d_model), lambda g, c: (g, 0)),
                pl.BlockSpec((1, local_n, GROUP), lambda g, c: (g, 0, 0)),
                pl.BlockSpec((GROUP, local_n), lambda g, c: (g, 0)),
                whole((local_n, d_model, d_ff), lambda g, c: (0, 0, 0)),
                whole((local_n, d_model, d_ff), lambda g, c: (0, 0, 0)),
                whole((local_n, d_ff, d_model), lambda g, c: (0, 0, 0)),
            ],
            out_specs=pl.BlockSpec((GROUP, d_model), lambda g, c: (g, 0)),
        ),
        compiler_params=pltpu.CompilerParams(vmem_limit_bytes=60 * 1024 * 1024),
        cost_estimate=pl.CostEstimate(
            flops=groups * TILE * 6 * d_model * d_ff,
            bytes_accessed=n_rows * d_model * 6,
            transcendentals=0,
        ),
    )(counts, x_rows, ranks, gates, wg_loc, wu_loc, wd_loc)


def solution(mesh):
    group_n = mesh.shape["ep"]
    row_spec = P(("dp", "ep"))
    expert_spec = P("ep")

    def local_step(tok_loc, route_loc, gate_loc, wg_loc, wu_loc, wd_loc):
        local_n = wg_loc.shape[0]
        tok_dev, d_model = tok_loc.shape
        n_experts = local_n * group_n
        chunk = tok_dev // CHUNKS
        groups = group_n * chunk // GROUP
        gathered = [
            lax.all_gather(tok_loc[c * chunk : (c + 1) * chunk], "ep", tiled=True) for c in range(CHUNKS)
        ]
        hit = route_loc[None, :, :] == jnp.arange(n_experts)[:, None, None]
        pair_gate = jnp.sum(jnp.where(hit, gate_loc[None], 0.0), axis=2)
        mine = lax.all_to_all(pair_gate.reshape(group_n, local_n, tok_dev), "ep", 0, 0, tiled=True)
        mine = mine.reshape(group_n, local_n, CHUNKS, chunk).transpose(2, 1, 0, 3)
        mine = mine.reshape(CHUNKS, local_n, groups, GROUP).transpose(0, 2, 1, 3)
        member = (mine > 0).astype(jnp.bfloat16)
        before = jnp.triu(jnp.ones((GROUP, GROUP), jnp.bfloat16))
        running = jnp.dot(member, before, preferred_element_type=jnp.float32).astype(jnp.int32)
        ranks = jnp.where(mine > 0, running - 1, -GROUP)
        counts = running[..., -1]
        gates = mine.transpose(0, 1, 3, 2).reshape(CHUNKS, groups * GROUP, local_n)

        outs = []
        for c in range(CHUNKS):
            partial = run_experts(gathered[c], ranks[c], gates[c], counts[c], wg_loc, wu_loc, wd_loc)
            outs.append(lax.psum_scatter(partial, "ep", scatter_dimension=0, tiled=True))
        return jnp.concatenate(outs, axis=0).astype(jnp.bfloat16)

    return jax.shard_map(
        local_step,
        mesh=mesh,
        in_specs=(row_spec, row_spec, row_spec, expert_spec, expert_spec, expert_spec),
        out_specs=row_spec,
        check_vma=False,
    )
```

```python
import functools

import jax
import jax.numpy as jnp
from jax import lax
from jax.experimental import pallas as pl
from jax.experimental.pallas import tpu as pltpu
from jax.sharding import PartitionSpec as P

CHUNKS = 4
GROUP = 1024
SMALL = 128
TILE = 256
COLS = 512


def expert_kernel(
    counts, x_ref, row_rank, col_rank, col_gate,
    wg_own, wu_own, wd_own, wg_peer, wu_peer, wd_peer,
    out_ref, wg_buf, wu_buf, wd_buf, acc, picked, w_sem, out_sem,
):
    group, expert = pl.program_id(0), pl.program_id(1)
    n_groups, n_experts = pl.num_programs(0), pl.num_programs(1)
    own_n = wg_own.shape[0]
    step = group * n_experts + expert
    slot = step % 2
    bufs = (wg_buf, wu_buf, wd_buf)

    def fetch(at, refs, index):
        for part, (ref, buf) in enumerate(zip(refs, bufs)):
            pltpu.make_async_copy(ref.at[index], buf.at[at % 2], w_sem.at[at % 2, part]).start()

    def fetch_step(at):
        index = at % n_experts

        @pl.when(index < own_n)
        def _():
            fetch(at, (wg_own, wu_own, wd_own), index)

        @pl.when(index >= own_n)
        def _():
            fetch(at, (wg_peer, wu_peer, wd_peer), index - own_n)

    def out_copy(at):
        rows = pl.ds(pl.multiple_of(at * GROUP, GROUP), GROUP)
        return pltpu.make_async_copy(acc, out_ref.at[rows], out_sem)

    @pl.when(step == 0)
    def _():
        fetch_step(step)

    @pl.when(step + 1 < n_groups * n_experts)
    def _():
        fetch_step(step + 1)

    @pl.when((expert == 0) & (group > 0))
    def _():
        out_copy(group - 1).wait()

    @pl.when(expert == 0)
    def _():
        acc[...] = jnp.zeros_like(acc)

    for part, (ref, buf) in enumerate(zip((wg_own, wu_own, wd_own), bufs)):
        pltpu.make_async_copy(ref.at[0], buf.at[slot], w_sem.at[slot, part]).wait()

    count = counts[group, expert]
    d_model = x_ref.shape[1]

    def run_tile(first, rows):
        row_id = lax.broadcasted_iota(jnp.int32, (rows, GROUP), 0)
        pick = jnp.where(row_id == row_rank[0, 0] - first, 1.0, 0.0).astype(jnp.bfloat16)
        for col in range(0, d_model, COLS):
            cols = slice(col, col + COLS)
            picked[:rows, cols] = jnp.dot(
                pick, x_ref[:, cols], preferred_element_type=jnp.float32
            ).astype(jnp.bfloat16)
        pre_gate = jnp.dot(picked[:rows, :], wg_buf[slot], preferred_element_type=jnp.float32)
        pre_up = jnp.dot(picked[:rows, :], wu_buf[slot], preferred_element_type=jnp.float32)
        hidden = (jax.nn.silu(pre_gate) * pre_up).astype(jnp.bfloat16)
        col_id = lax.broadcasted_iota(jnp.int32, (GROUP, rows), 1)
        put = jnp.where(col_id == col_rank[0] - first, 1.0, 0.0).astype(jnp.bfloat16)
        gate = col_gate[0]
        for col in range(0, d_model, COLS):
            cols = slice(col, col + COLS)
            rows_out = jnp.dot(hidden, wd_buf[slot, :, cols], preferred_element_type=jnp.float32)
            placed = jnp.dot(put, rows_out.astype(jnp.bfloat16), preferred_element_type=jnp.float32)
            acc[:, cols] += gate * placed

    @pl.when((count > 0) & (count <= SMALL))
    def _():
        run_tile(0, SMALL)

    @pl.when(count > SMALL)
    def _():
        def body(tile, carry):
            run_tile(tile * TILE, TILE)
            return carry

        lax.fori_loop(0, (count + TILE - 1) // TILE, body, 0)

    @pl.when(expert == n_experts - 1)
    def _():
        out_copy(group).start()

    @pl.when((expert == n_experts - 1) & (group == n_groups - 1))
    def _():
        out_copy(group).wait()


def run_experts(x_rows, ranks, gates, counts, own, peer):
    n_rows, d_model = x_rows.shape
    n_groups, n_experts = counts.shape
    d_ff = own[0].shape[2]
    hbm = pl.BlockSpec(memory_space=pl.ANY)
    column = pl.BlockSpec((1, GROUP, 1), lambda g, e, c: (e, g, 0))
    return pl.pallas_call(
        expert_kernel,
        out_shape=jax.ShapeDtypeStruct((n_rows, d_model), jnp.float32),
        grid_spec=pltpu.PrefetchScalarGridSpec(
            num_scalar_prefetch=1,
            grid=(n_groups, n_experts),
            in_specs=[
                pl.BlockSpec((GROUP, d_model), lambda g, e, c: (g, 0), pipeline_mode=pl.Buffered(1)),
                pl.BlockSpec((1, 1, 1, GROUP), lambda g, e, c: (e, g, 0, 0)),
                column,
                column,
            ]
            + [hbm] * 6,
            out_specs=hbm,
            scratch_shapes=[
                pltpu.VMEM((2, d_model, d_ff), jnp.bfloat16),
                pltpu.VMEM((2, d_model, d_ff), jnp.bfloat16),
                pltpu.VMEM((2, d_ff, d_model), jnp.bfloat16),
                pltpu.VMEM((GROUP, d_model), jnp.float32),
                pltpu.VMEM((TILE, d_model), jnp.bfloat16),
                pltpu.SemaphoreType.DMA((2, 3)),
                pltpu.SemaphoreType.DMA,
            ],
        ),
        compiler_params=pltpu.CompilerParams(vmem_limit_bytes=62 * 1024 * 1024),
        cost_estimate=pl.CostEstimate(
            flops=n_rows * 6 * d_model * d_ff, bytes_accessed=n_rows * d_model * 6, transcendentals=0
        ),
    )(
        counts,
        x_rows,
        ranks.reshape(n_experts, n_groups, 1, GROUP),
        ranks.reshape(n_experts, n_rows, 1),
        gates.reshape(n_experts, n_rows, 1),
        *own,
        *peer,
    )


def solution(mesh):
    group_n = mesh.shape["ep"]
    row_spec = P(("dp", "ep"))
    expert_spec = P("ep")
    pairs = [(j, j ^ 1) for j in range(group_n)]
    sides = [list(range(side, group_n, 2)) for side in range(2)]
    homes = group_n // 2

    def local_step(tok_loc, route_loc, gate_loc, wg_loc, wu_loc, wd_loc):
        own = (wg_loc, wu_loc, wd_loc)
        peer = tuple(lax.ppermute(w, "ep", pairs) for w in own)
        own_n = wg_loc.shape[0]
        shared_n = 2 * own_n
        tok_dev, d_model = tok_loc.shape
        n_experts = own_n * group_n
        chunk = tok_dev // CHUNKS
        n_groups = homes * chunk // GROUP
        gathered = [
            lax.all_gather(tok_loc[c * chunk : (c + 1) * chunk], "ep", tiled=True, axis_index_groups=sides)
            for c in range(CHUNKS)
        ]
        hit = route_loc[None, :, :] == jnp.arange(n_experts)[:, None, None]
        pair_gate = jnp.sum(jnp.where(hit, gate_loc[None], 0.0), axis=2)
        mine = lax.all_to_all(
            pair_gate.reshape(homes, shared_n, tok_dev), "ep", 0, 0, axis_index_groups=sides, tiled=True
        )
        mine = mine.reshape(homes, shared_n, CHUNKS, chunk).transpose(2, 1, 0, 3)
        mine = mine.reshape(CHUNKS, shared_n, n_groups, GROUP)
        mine = jnp.where(lax.axis_index("ep") % 2 == 0, mine, jnp.roll(mine, own_n, axis=1))
        member = (mine > 0).astype(jnp.bfloat16)
        before = jnp.triu(jnp.ones((GROUP, GROUP), jnp.bfloat16))
        running = jnp.dot(member, before, preferred_element_type=jnp.float32).astype(jnp.int32)
        ranks = jnp.where(mine > 0, running - 1, -GROUP)
        counts = running[..., -1].transpose(0, 2, 1)

        outs = []
        for c in range(CHUNKS):
            partial = run_experts(gathered[c], ranks[c], mine[c], counts[c], own, peer)
            outs.append(
                lax.psum_scatter(partial, "ep", scatter_dimension=0, tiled=True, axis_index_groups=sides)
            )
        return jnp.concatenate(outs, axis=0).astype(jnp.bfloat16)

    return jax.shard_map(
        local_step,
        mesh=mesh,
        in_specs=(row_spec, row_spec, row_spec, expert_spec, expert_spec, expert_spec),
        out_specs=row_spec,
        check_vma=False,
    )
```

```python
import functools

import jax
import jax.numpy as jnp
from jax import lax
from jax.experimental import pallas as pl
from jax.experimental.pallas import tpu as pltpu
from jax.sharding import PartitionSpec as P

ROWS = 64
GATHERS = (3, 5)
SCATTERS = (3, 3, 2)
SMALL = 128
TILE = 512
COLS = 512


def expert_kernel(
    counts, x_ref, pair_ref,
    wg_own, wu_own, wd_own, wg_peer, wu_peer, wd_peer,
    out_ref, wg_buf, wu_buf, wd_buf, acc, picked, w_sem, out_sem,
):
    group, expert = pl.program_id(0), pl.program_id(1)
    n_groups, n_experts = pl.num_programs(0), pl.num_programs(1)
    own_n = wg_own.shape[0]
    step = group * n_experts + expert
    slot = step % 2
    bufs = (wg_buf, wu_buf, wd_buf)
    homes, home_rows, d_model = x_ref.shape
    n_rows = homes * home_rows

    def fetch(at, refs, index):
        for part, (ref, buf) in enumerate(zip(refs, bufs)):
            pltpu.make_async_copy(ref.at[index], buf.at[at % 2], w_sem.at[at % 2, part]).start()

    def fetch_step(at):
        index = at % n_experts

        @pl.when(index < own_n)
        def _():
            fetch(at, (wg_own, wu_own, wd_own), index)

        @pl.when(index >= own_n)
        def _():
            fetch(at, (wg_peer, wu_peer, wd_peer), index - own_n)

    def out_copy(at):
        rows = pl.ds(pl.multiple_of(at * home_rows, home_rows), home_rows)
        return pltpu.make_async_copy(acc, out_ref.at[:, rows], out_sem)

    @pl.when(step == 0)
    def _():
        fetch_step(step)

    @pl.when(step + 1 < n_groups * n_experts)
    def _():
        fetch_step(step + 1)

    @pl.when((expert == 0) & (group > 0))
    def _():
        out_copy(group - 1).wait()

    @pl.when(expert == 0)
    def _():
        acc[...] = jnp.zeros_like(acc)

    for part, (ref, buf) in enumerate(zip((wg_own, wu_own, wd_own), bufs)):
        pltpu.make_async_copy(ref.at[0], buf.at[slot], w_sem.at[slot, part]).wait()

    count = counts[group, expert]

    def run_tile(first, rows):
        row_rank = pair_ref[0, pl.ds(expert, 1), :] - first
        row_id = lax.broadcasted_iota(jnp.int32, (rows, n_rows), 0).astype(jnp.float32)
        pick = jnp.where(row_id == row_rank, 1.0, 0.0).astype(jnp.bfloat16)
        for col in range(0, d_model, COLS):
            cols = slice(col, col + COLS)
            picked[:rows, cols] = jnp.dot(
                pick, x_ref[:, :, cols].reshape(n_rows, COLS), preferred_element_type=jnp.float32
            ).astype(jnp.bfloat16)
        pre_gate = jnp.dot(picked[:rows, :], wg_buf[slot], preferred_element_type=jnp.float32)
        pre_up = jnp.dot(picked[:rows, :], wu_buf[slot], preferred_element_type=jnp.float32)
        hidden = (jax.nn.silu(pre_gate) * pre_up).astype(jnp.bfloat16)
        pair = jnp.transpose(pair_ref[0])
        lane = lax.broadcasted_iota(jnp.int32, pair.shape, 1)
        col_rank = jnp.sum(jnp.where(lane == expert, pair, 0.0), axis=1, keepdims=True) - first
        gate = jnp.sum(jnp.where(lane == expert + n_experts, pair, 0.0), axis=1, keepdims=True)
        col_id = lax.broadcasted_iota(jnp.int32, (n_rows, rows), 1).astype(jnp.float32)
        put = jnp.where(col_id == col_rank, 1.0, 0.0).astype(jnp.bfloat16)
        for col in range(0, d_model, COLS):
            cols = slice(col, col + COLS)
            rows_out = jnp.dot(hidden, wd_buf[slot, :, cols], preferred_element_type=jnp.float32)
            placed = jnp.dot(put, rows_out.astype(jnp.bfloat16), preferred_element_type=jnp.float32)
            acc[:, :, cols] += (gate * placed).reshape(homes, home_rows, COLS)

    @pl.when((count > 0) & (count <= SMALL))
    def _():
        run_tile(0.0, SMALL)

    @pl.when(count > SMALL)
    def _():
        def body(tile, carry):
            run_tile((tile * TILE).astype(jnp.float32), TILE)
            return carry

        lax.fori_loop(0, (count + TILE - 1) // TILE, body, 0)

    @pl.when(expert == n_experts - 1)
    def _():
        out_copy(group).start()

    @pl.when((expert == n_experts - 1) & (group == n_groups - 1))
    def _():
        out_copy(group).wait()


def run_experts(x_rows, at, pairs, counts, own, peer):
    homes, _, d_model = x_rows.shape
    n_groups, n_experts = counts.shape
    d_ff = own[0].shape[2]
    hbm = pl.BlockSpec(memory_space=pl.ANY)
    return pl.pallas_call(
        expert_kernel,
        out_shape=jax.ShapeDtypeStruct((homes, n_groups * ROWS, d_model), jnp.float32),
        grid_spec=pltpu.PrefetchScalarGridSpec(
            num_scalar_prefetch=1,
            grid=(n_groups, n_experts),
            in_specs=[
                pl.BlockSpec(
                    (homes, ROWS, d_model), lambda g, e, c: (0, g + at, 0), pipeline_mode=pl.Buffered(1)
                ),
                pl.BlockSpec((1,) + pairs.shape[1:], lambda g, e, c: (g, 0, 0)),
            ]
            + [hbm] * 6,
            out_specs=hbm,
            scratch_shapes=[
                pltpu.VMEM((2, d_model, d_ff), jnp.bfloat16),
                pltpu.VMEM((2, d_model, d_ff), jnp.bfloat16),
                pltpu.VMEM((2, d_ff, d_model), jnp.bfloat16),
                pltpu.VMEM((homes, ROWS, d_model), jnp.float32),
                pltpu.VMEM((TILE, d_model), jnp.bfloat16),
                pltpu.SemaphoreType.DMA((2, 3)),
                pltpu.SemaphoreType.DMA,
            ],
        ),
        compiler_params=pltpu.CompilerParams(vmem_limit_bytes=67_000_000),
        cost_estimate=pl.CostEstimate(
            flops=n_groups * homes * ROWS * 6 * d_model * d_ff,
            bytes_accessed=n_groups * homes * ROWS * d_model * 6,
            transcendentals=0,
        ),
    )(counts, x_rows, pairs, *own, *peer)


def solution(mesh):
    group_n = mesh.shape["ep"]
    row_spec = P(("dp", "ep"))
    expert_spec = P("ep")
    pairs = [(j, j ^ 1) for j in range(group_n)]
    sides = [list(range(side, group_n, 2)) for side in range(2)]
    homes = group_n // 2

    def local_step(tok_loc, route_loc, gate_loc, wg_loc, wu_loc, wd_loc):
        own = (wg_loc, wu_loc, wd_loc)
        peer = tuple(lax.ppermute(w, "ep", pairs) for w in own)
        own_n = wg_loc.shape[0]
        shared_n = 2 * own_n
        tok_dev, d_model = tok_loc.shape
        n_experts = own_n * group_n
        n_groups = tok_dev // ROWS
        assert sum(GATHERS) == sum(SCATTERS) == n_groups
        placed_at = []
        for groups in GATHERS:
            first = len(placed_at) * ROWS
            rows = lax.all_gather(tok_loc[first : first + groups * ROWS], "ep", axis_index_groups=sides)
            placed_at += [(rows, at) for at in range(groups)]
        hit = route_loc[None, :, :] == jnp.arange(n_experts)[:, None, None]
        pair_gate = jnp.sum(jnp.where(hit, gate_loc[None], 0.0), axis=2)
        mine = lax.all_to_all(
            pair_gate.reshape(homes, shared_n, tok_dev), "ep", 0, 0, axis_index_groups=sides, tiled=True
        )
        mine = mine.reshape(homes, shared_n, n_groups, ROWS).transpose(2, 1, 0, 3)
        mine = mine.reshape(n_groups, shared_n, homes * ROWS)
        mine = jnp.where(lax.axis_index("ep") % 2 == 0, mine, jnp.roll(mine, own_n, axis=1))
        member = (mine > 0).astype(jnp.bfloat16)
        before = jnp.triu(jnp.ones((homes * ROWS, homes * ROWS), jnp.bfloat16))
        running = jnp.dot(member, before, preferred_element_type=jnp.float32)
        ranks = jnp.where(mine > 0, running - 1, -1.0)
        counts = running[..., -1].astype(jnp.int32)
        table = jnp.concatenate([ranks, mine], axis=1)

        outs = []
        first = 0
        for groups in SCATTERS:
            rows, at = placed_at[first]
            span = slice(first, first + groups)
            partial = run_experts(rows, at, table[span], counts[span], own, peer)
            partial = partial.reshape(homes * groups * ROWS, d_model)
            outs.append(
                lax.psum_scatter(partial, "ep", scatter_dimension=0, tiled=True, axis_index_groups=sides)
            )
            first += groups
        return jnp.concatenate(outs, axis=0).astype(jnp.bfloat16)

    return jax.shard_map(
        local_step,
        mesh=mesh,
        in_specs=(row_spec, row_spec, row_spec, expert_spec, expert_spec, expert_spec),
        out_specs=row_spec,
        check_vma=False,
    )
```
